32 devices in a mesh: gx: 4 (over z), gy: 8 (over y, x, core).
Axes of the slice: x: 2, y: 2, z: 4, core: 2. Of those that a mesh axis runs over, the one named last changes fastest.
Arguments:
- factor: bfloat16 [256, 256, 768], P(('gx', 'gy')), may hold values from -0.21875 to 0.21875
- right_sides: bfloat16 [65536, 128], P(('gx', 'gy')), may hold values from -6 to 6
- send_rows: int32 [32, 32, 48], P(('gx', 'gy')), may hold values from 0 to 2047, as said below
- neighbour_slot: int32 [256, 512], P(('gx', 'gy')), may hold values from 0 to 1536, as said below
Outputs:
- half_product: bfloat16 [65536, 128], P(('gx', 'gy'))
- full_product: bfloat16 [65536, 128], P(('gx', 'gy'))
The draws below stay inside these ranges and needn't reach their ends.
Inputs may be any that keep to these rules, and one draw needn't show every extreme that they name: `send_rows`: devices follow an ordering drawn with the tables, and device d receives only from owners e that precede it. For each owner e and receiver d the first c[d, e] places hold distinct rows and the rest hold 0, where c[d, e] is at most 48; every device but the first in the ordering receives 48 rows from the owner just before it, and the c[d, e] of one receiver sum to at most 1024. `neighbour_slot`: an entry is either a live place (p below c[d, e]) or 1536, which marks padding; the live entries of one block are distinct, and every live place of a device is named by exactly 4 of that device's blocks.
All inputs are finite; a program needn't handle non-finite values.
Results may differ from the reference program's by a relative error of at most 0.0047.
Values may be sent and summed in bfloat16 or wider, within the bound.
A program may use at most 64 MiB of HBM per device.

```python
import jax
import jax.numpy as jnp
from jax import lax

BLOCK = 256
NBRS = 512
BLK_DEV = 8
RHS = 128
ROUNDS = 1
USES = 4
NBLK = 256
ROWS_DEV = 2048
NROWS = 65536
PAIR_MEAN = 32
CAP = 48
N_GX = 4
N_GY = 8
DEVICES = 32


def plan_tables(key):
    folded = jax.random.fold_in(key, 11)
    subkeys = jax.random.split(folded, 4 + USES)
    needed = BLK_DEV * NBRS // USES
    half_range = PAIR_MEAN // 2
    ranking = jax.random.permutation(subkeys[0], DEVICES).astype(jnp.int32)
    rank_gap = ranking[:, None] - ranking[None, :]
    raw_counts = PAIR_MEAN + jax.random.randint(subkeys[1], (DEVICES, DEVICES), -half_range, half_range + 1)
    raw_counts = jnp.where(rank_gap == 1, CAP, raw_counts)
    raw_counts = jnp.where(rank_gap > 0, raw_counts, 0).astype(jnp.int32)
    order_key = jnp.where(rank_gap > 0, rank_gap, DEVICES + 1)
    ordering_owners = jnp.argsort(order_key, axis=1, stable=True)
    sorted_counts = jnp.take_along_axis(raw_counts, ordering_owners, axis=1)
    before_sorted = jnp.cumsum(sorted_counts, axis=1) - sorted_counts
    inverse_order = jnp.argsort(ordering_owners, axis=1, stable=True)
    before = jnp.take_along_axis(before_sorted, inverse_order, axis=1)
    counts = jnp.clip(needed - before, 0, raw_counts).astype(jnp.int32)
    live_total = jnp.sum(counts, axis=1)
    places = jnp.arange(CAP)
    is_live = places[None, None, :] < counts[:, :, None]
    live_flat = is_live.reshape(DEVICES, DEVICES * CAP)
    width_all = DEVICES * CAP
    spread = 2 ** 30 // width_all
    positions = jnp.arange(needed)[None, :]
    groups = []
    for use_index in range(USES):
        random_part = jax.random.randint(subkeys[4 + use_index], (DEVICES, width_all), 0, spread)
        scores = random_part * width_all + jnp.arange(width_all)[None, :] + jnp.where(live_flat, 0, 2 ** 30)
        ordering = jnp.argsort(scores, axis=1, stable=True)[:, :needed]
        ordering = jnp.where(positions < live_total[:, None], ordering, width_all)
        groups.append(ordering.reshape(DEVICES, BLK_DEV // USES, NBRS))
    neighbour_table = jnp.stack(groups, axis=1).reshape(DEVICES * BLK_DEV, NBRS).astype(jnp.int32)
    starts = jax.random.randint(subkeys[2], (DEVICES, DEVICES, 1), 0, ROWS_DEV)
    strides = 2 * jax.random.randint(subkeys[3], (DEVICES, DEVICES, 1), 0, ROWS_DEV // 2) + 1
    row_choice = (starts + places[None, None, :] * strides) % ROWS_DEV
    send_table = jnp.where(jnp.transpose(is_live, (1, 0, 2)), row_choice, 0).astype(jnp.int32)
    return (send_table, neighbour_table)


def draw_send_rows(key, part):
    return plan_tables(key)[0]


def draw_neighbour_slot(key, part):
    return plan_tables(key)[1]


def block_levels(own_key, extent, pieces, least, largest):
    factor_of = 1.0
    for dim, parts in pieces:
        draws = jax.random.uniform(jax.random.fold_in(jax.random.fold_in(own_key, 6), dim), (parts,), jnp.float32, least / len(pieces), largest / len(pieces))
        factor_of = factor_of * jnp.repeat(jnp.exp(draws), extent[dim] // parts).reshape((-1,) + (1,) * (len(extent) - 1 - dim))
    return factor_of


def scatter_about(own_key, shape, scale, reach, shards=(), kind=jnp.bfloat16):
    gain = block_levels(own_key, shape, shards, -0.22, 0.18) if shards else 1.0
    array = jax.random.normal(own_key, shape, jnp.float32) * scale * gain
    return jnp.minimum(jnp.maximum(array, -reach), reach).astype(kind)


def setup_inputs(seed: int = 0) -> dict:
    key_of = jax.random.split(jax.random.key(seed), 5)
    return {
        "factor": scatter_about(key_of[0], (NBLK, BLOCK, BLOCK + NBRS), (BLOCK + NBRS) ** -0.5, 0.21875, ((0, 32),)),
        "right_sides": scatter_about(key_of[1], (NROWS, RHS), 1.0, 6.0, ((0, 32),)),
        "send_rows": draw_send_rows(jax.random.fold_in(key_of[4], 71), 0),
        "neighbour_slot": draw_neighbour_slot(jax.random.fold_in(key_of[4], 71), 0),
    }


def reference(factor, right_sides, send_rows, neighbour_slot):
    devices = N_GX * N_GY
    rows_dev = BLK_DEV * BLOCK
    sentinel = devices * CAP
    is_live = neighbour_slot < sentinel
    safe_slot = jnp.where(is_live, neighbour_slot, 0).astype(jnp.int32)
    owner_dev = safe_slot // CAP
    place_in = safe_slot % CAP
    requester = (jnp.arange(NBLK, dtype=jnp.int32) // BLK_DEV)[:, None]
    local_row = send_rows[owner_dev, requester, place_in]
    global_ids = (owner_dev * rows_dev + local_row).astype(jnp.int32)
    offsets = jnp.repeat(jnp.arange(devices, dtype=jnp.int32) * rows_dev, CAP)
    slot_rows = (jnp.transpose(send_rows, (1, 0, 2)).reshape(devices, devices * CAP) + offsets[None, :]).astype(jnp.int32)
    factor_dev = factor.reshape(devices, BLK_DEV, BLOCK, BLOCK + NBRS)
    ids_dev = global_ids.reshape(devices, BLK_DEV, NBRS)
    live_dev = is_live.reshape(devices, BLK_DEV, NBRS)
    slots_dev = neighbour_slot.reshape(devices, BLK_DEV * NBRS)

    def one_round(vector):
        def device_step(summed, inputs):
            dev_factor, dev_ids, dev_live, dev_slots, dev_rows, dev_index = inputs
            first_row = (dev_index * rows_dev).astype(jnp.int32)
            own_rows = lax.dynamic_slice_in_dim(vector, first_row, rows_dev, 0).reshape(BLK_DEV, BLOCK, RHS)
            fetched = vector[dev_ids]
            fetched = jnp.where(dev_live[:, :, None], fetched, jnp.zeros_like(fetched))
            stacked = jnp.concatenate([own_rows, fetched], axis=1).astype(jnp.float32)
            factor32 = dev_factor.astype(jnp.float32)
            z_block = jnp.einsum("bij,bjr->bir", factor32, stacked).astype(jnp.bfloat16)
            z_again = lax.optimization_barrier(z_block).astype(jnp.float32)
            backward = jnp.einsum("bij,bir->bjr", factor32, z_again)
            own_back = backward[:, :BLOCK].reshape(rows_dev, RHS)
            slot_sum = jax.ops.segment_sum(backward[:, BLOCK:].reshape(BLK_DEV * NBRS, RHS), dev_slots, num_segments=devices * CAP + 1)[:devices * CAP]
            slot_sum = lax.optimization_barrier(slot_sum.astype(jnp.bfloat16)).astype(jnp.float32)
            summed = summed.at[dev_rows].add(slot_sum)
            current = lax.dynamic_slice_in_dim(summed, first_row, rows_dev, 0)
            summed = lax.dynamic_update_slice_in_dim(summed, current + own_back, first_row, 0)
            return summed, z_block.reshape(rows_dev, RHS)

        start_sum = jnp.zeros((NROWS, RHS), jnp.float32)
        summed, z_rows = lax.scan(device_step, start_sum, (factor_dev, ids_dev, live_dev, slots_dev, slot_rows, jnp.arange(devices, dtype=jnp.int32)))
        return z_rows.reshape(NROWS, RHS), summed.astype(jnp.bfloat16)

    vector = right_sides
    weighted = right_sides
    for round_index in range(ROUNDS):
        weighted, vector = one_round(vector)
    return weighted, vector
```

```python
import functools

import jax
import jax.numpy as jnp
from jax import lax
from jax.experimental import pallas as pl
from jax.experimental.pallas import tpu as pltpu
from jax.sharding import PartitionSpec as P

MESH = pl.DeviceIdType.MESH
NT = (((1,), (1,)), ((), ()))
TN = (((0,), (0,)), ((), ()))


def one_hot(mask):
    return jnp.where(mask, 1.0, 0.0).astype(jnp.bfloat16)


def orders(outer):
    split = outer // 2

    def crosses(a, b):
        return (a < split) != (b < split)

    middle = (outer - 1) / 2
    rows, sums, waits = [], [], []
    for a in range(outer):
        every = range(outer)
        rows.append(sorted(every, key=lambda b: (abs(b - middle), not crosses(a, b), b)))
        sums.append(sorted(every, key=lambda b: (b != 0, not crosses(a, b), b == a, b)))
        waits.append(sorted((b for b in every if b != a), key=lambda b: (abs(b - a), b)))
    return rows, sums, waits


def kernel(
    outer, inner, tile,
    factor_ref, vector_ref, table_ref, slots_ref, half, full,
    factor, vector, table, slots, spread, spread_t, picker, packed, received, sums, returned,
    id_rows, id_columns, slot_columns, total, wide,
    load_sem, go_sem, back_go_sem, come_sem, back_come_sem,
):
    blocks, width, _ = factor.shape
    pairs, _ = vector.shape
    columns = half.shape[1]
    senders, capacity, _ = packed.shape
    places = senders * capacity
    span = inner * capacity
    far_width = slots.shape[1]
    side_blocks = blocks // 2
    gx, gy = lax.axis_index("gx"), lax.axis_index("gy")
    me = gx * inner + gy
    row_order, sum_order, wait_order = orders(outer)

    barrier = pltpu.get_barrier_semaphore()

    def greet(k, carry):
        other = lax.rem(me + k, senders)
        pl.semaphore_signal(
            barrier, inc=1, device_id=(other // inner, lax.rem(other, inner)), device_id_type=MESH
        )
        return carry

    loads = [
        pltpu.make_async_copy(table_ref, table, load_sem.at[0]),
        pltpu.make_async_copy(
            vector_ref.at[pl.ds(0, pairs)], vector.at[:, pl.ds(0, columns)], load_sem.at[1]
        ),
        pltpu.make_async_copy(
            vector_ref.at[pl.ds(pairs, pairs)], vector.at[:, pl.ds(columns, columns)], load_sem.at[2]
        ),
        pltpu.make_async_copy(slots_ref, slots, load_sem.at[3]),
        pltpu.make_async_copy(factor_ref, factor, load_sem.at[4]),
    ]
    for load in loads:
        load.start()
    lax.fori_loop(1, senders, greet, 0)

    received[me] = jnp.zeros((capacity, columns), jnp.bfloat16)
    returned[me] = jnp.zeros((capacity, columns), jnp.bfloat16)

    def listed(lists, k):
        plane = jnp.int32(lists[outer - 1][k])
        for i in range(outer - 1):
            plane = jnp.where(gx == i, jnp.int32(lists[i][k]), plane)
        return plane

    def group_places(g):
        return pl.ds(pl.multiple_of(g * span, 128), span)

    def group(ref, g):
        return ref[pl.ds(g * inner, inner)].reshape(span, columns)

    def send_group(source, target, send_sem, recv_sem, plane):
        def step(y, carry):
            to_y = lax.rem(gy + y, inner)
            pltpu.make_async_remote_copy(
                src_ref=source.at[plane * inner + to_y],
                dst_ref=target.at[me],
                send_sem=send_sem,
                recv_sem=recv_sem.at[gx],
                device_id=(plane, to_y),
                device_id_type=MESH,
            ).start()
            return carry

        lax.fori_loop(jnp.where(plane == gx, 1, 0), inner, step, 0)

    def await_bytes(buffer, sem, slabs):
        whole = buffer.at[pl.ds(0, slabs)]
        pltpu.make_async_copy(whole, whole, sem).wait()

    outward = (packed, received, go_sem, come_sem)
    inward = (sums, returned, back_go_sem, back_come_sem)

    loads[0].wait()
    flipped = table[0].T
    for e in range(senders):
        id_columns[pl.ds(e * capacity, capacity), :] = jnp.broadcast_to(
            flipped[:, e : e + 1], (capacity, 128)
        )
    loads[1].wait()
    loads[2].wait()

    def lanes(ids, n):
        return jnp.concatenate([ids] * (n // 128), axis=1)

    def pack(g):
        part = span // 2
        for r in range(2):
            ids = id_columns[pl.ds(pl.multiple_of(g * span + r * part, 8), part), :]
            upper = ids >= pairs
            ids = lanes(jnp.where(upper, ids - pairs, ids), tile)
            lane = lax.broadcasted_iota(jnp.int32, (part, tile), 1)
            rows = jnp.zeros((part, 2 * columns), jnp.float32)
            for c in range(pairs // tile):
                rows = rows + jnp.dot(
                    one_hot(ids == lane + c * tile),
                    vector[c * tile : (c + 1) * tile, :],
                    preferred_element_type=jnp.float32,
                )
            upper = lanes(upper.astype(jnp.int32), columns) > 0
            picked = jnp.where(upper, rows[:, columns:], rows[:, :columns])
            packed[pl.ds(g * inner + r * (inner // 2), inner // 2)] = picked.astype(
                jnp.bfloat16
            ).reshape(inner // 2, capacity, columns)

    for k in range(outer):
        plane = listed(row_order, k)
        pack(plane)
        if k == 0:
            pl.semaphore_wait(barrier, senders - 1)
        send_group(*outward, plane)

    loads[3].wait()
    slots_t = slots[...].T
    for b in range(blocks):
        slot_columns[b * far_width : (b + 1) * far_width, :] = jnp.broadcast_to(
            slots_t[:, b : b + 1], (far_width, 128)
        )
    loads[4].wait()

    def rows_of(side, b):
        return pl.ds(pl.multiple_of(b * width, width), width), slice(side * columns, (side + 1) * columns)

    def spread_block(side):
        def step(n, carry):
            b = side * side_blocks + n
            here = pl.ds(pl.multiple_of(b * width, width), width)
            far = factor[b, :, width:]
            ids = slots[pl.ds(b, 1), :]
            down = slot_columns[pl.ds(pl.multiple_of(b * far_width, 128), far_width), :]
            down = lanes(down, tile)
            lane = lax.broadcasted_iota(jnp.int32, (far_width, tile), 1)
            for c in range(places // tile):
                place = lax.broadcasted_iota(jnp.int32, (tile, far_width), 0) + c * tile
                there = slice(c * tile, (c + 1) * tile)
                spread_t[there, here] = lax.dot_general(
                    one_hot(ids == place), far, NT, preferred_element_type=jnp.float32
                ).astype(jnp.bfloat16)
                spread[here, there] = jnp.dot(
                    far, one_hot(down == lane + c * tile), preferred_element_type=jnp.float32
                ).astype(jnp.bfloat16)
            total[here, :] = jnp.dot(
                factor[b, :, :width], vector[rows_of(side, n)], preferred_element_type=jnp.float32
            )
            return carry

        lax.fori_loop(0, side_blocks, step, 0)

    for side in range(2):
        spread_block(side)

    id_rows[...] = jnp.concatenate([table[0, e : e + 1, :] for e in range(senders)], axis=1)
    id_rows[...] = jnp.where(id_rows[...] >= pairs, id_rows[...] - pairs, id_rows[...])

    def pick_rows(n, carry):
        here = pl.ds(pl.multiple_of(n * width, width), width)
        row = lax.broadcasted_iota(jnp.int32, (width, places), 0) + n * width
        picker[here, :] = one_hot(id_rows[0:1, :] == row)
        return carry

    lax.fori_loop(0, pairs // width, pick_rows, 0)

    slab = half.shape[0] // 2
    for n in range(outer):
        if n == 0:
            g = gx
            await_bytes(received, come_sem.at[g], inner - 1)
        else:
            g = listed(wait_order, n - 1)
            await_bytes(received, come_sem.at[g], inner)
        rows = group(received, g)
        for h in range(2):
            part = pl.ds(h * slab, slab)
            value = total[part, :] + jnp.dot(
                spread[part, group_places(g)], rows, preferred_element_type=jnp.float32
            )
            if n < outer - 1:
                total[part, :] = value
            else:
                half[part, :] = value.astype(jnp.bfloat16)

    for k in range(outer):
        g = listed(sum_order, k)
        value = jnp.dot(
            spread_t[pl.ds(pl.multiple_of(g * span, 128), span), :], half[...],
            preferred_element_type=jnp.float32,
        )
        sums[pl.ds(g * inner, inner)] = value.astype(jnp.bfloat16).reshape(inner, capacity, columns)
        send_group(*inward, g)

    def own_block(side):
        def step(n, carry):
            b = side * side_blocks + n
            here = pl.ds(pl.multiple_of(b * width, width), width)
            wide[rows_of(side, n)] = lax.dot_general(
                factor[b, :, :width], half[here, :], TN, preferred_element_type=jnp.float32
            )
            return carry

        lax.fori_loop(0, side_blocks, step, 0)

    for side in range(2):
        own_block(side)
    await_bytes(packed, go_sem, senders - 1)

    for n in range(outer):
        if n == 0:
            g = gx
            await_bytes(returned, back_come_sem.at[g], inner - 1)
        else:
            g = listed(wait_order, n - 1)
            await_bytes(returned, back_come_sem.at[g], inner)
        rows = group(returned, g)
        upper = lanes(id_columns[pl.ds(pl.multiple_of(g * span, 8), span), :], columns) >= pairs
        none = jnp.zeros_like(rows)
        both = jnp.concatenate([jnp.where(upper, none, rows), jnp.where(upper, rows, none)], axis=1)
        for h in range(2):
            part = pl.ds(h * (pairs // 2), pairs // 2)
            value = wide[part, :] + jnp.dot(
                picker[part, group_places(g)], both, preferred_element_type=jnp.float32
            )
            if n < outer - 1:
                wide[part, :] = value
            else:
                value = value.astype(jnp.bfloat16)
                full[part, :] = value[:, :columns]
                full[pl.ds(pairs + h * (pairs // 2), pairs // 2), :] = value[:, columns:]
    await_bytes(sums, back_go_sem, senders - 1)


def write_out(half_ref, full_ref, half_out, full_out, sems):
    copies = [
        pltpu.make_async_copy(half_ref, half_out, sems.at[0]),
        pltpu.make_async_copy(full_ref, full_out, sems.at[1]),
    ]
    for copy in copies:
        copy.start()
    for copy in copies:
        copy.wait()


def fused(factor, right_sides, send_rows, neighbour_slot, tile):
    blocks, width, _ = factor.shape
    rows_here, columns = right_sides.shape
    _, senders, capacity = send_rows.shape
    places = senders * capacity
    outer, inner = lax.axis_size("gx"), lax.axis_size("gy")
    kept = jnp.bfloat16
    out = pltpu.VMEM((rows_here, columns), kept)
    moved = pltpu.VMEM((senders, capacity, columns), kept)
    pairs, far_width = rows_here // 2, neighbour_slot.shape[1]
    flag, flags = pltpu.SemaphoreType.DMA, pltpu.SemaphoreType.DMA((outer,))
    half, full = pl.pallas_call(
        functools.partial(kernel, outer, inner, tile),
        out_shape=(out, out),
        in_specs=[pl.BlockSpec(memory_space=pl.ANY)] * 4,
        out_specs=(pl.BlockSpec(memory_space=pltpu.VMEM),) * 2,
        scratch_shapes=[
            pltpu.VMEM(factor.shape, kept),
            pltpu.VMEM((pairs, 2 * columns), kept),
            pltpu.VMEM(send_rows.shape, jnp.int32),
            pltpu.VMEM(neighbour_slot.shape, jnp.int32),
            pltpu.VMEM((rows_here, places), kept),
            pltpu.VMEM((places, rows_here), kept),
            pltpu.VMEM((pairs, places), kept),
            moved, moved, moved, moved,
            pltpu.VMEM((1, places), jnp.int32),
            pltpu.VMEM((places, 128), jnp.int32),
            pltpu.VMEM((blocks * far_width, 128), jnp.int32),
            pltpu.VMEM((rows_here, columns), jnp.float32),
            pltpu.VMEM((pairs, 2 * columns), jnp.float32),
            pltpu.SemaphoreType.DMA((5,)),
            flag, flag, flags, flags,
        ],
        compiler_params=pltpu.CompilerParams(collective_id=0, has_side_effects=True),
    )(factor, right_sides, send_rows, neighbour_slot)
    written = jax.ShapeDtypeStruct((rows_here, columns), kept)
    return pl.pallas_call(
        write_out,
        out_shape=(written, written),
        in_specs=[pl.BlockSpec(memory_space=pltpu.VMEM)] * 2,
        out_specs=(pl.BlockSpec(memory_space=pl.ANY),) * 2,
        scratch_shapes=[pltpu.SemaphoreType.DMA((2,))],
        compiler_params=pltpu.CompilerParams(vmem_limit_bytes=1 << 20),
    )(half, full)


def move_rows(packed):
    moved = lax.all_to_all(
        lax.all_to_all(packed, "gy", split_axis=1, concat_axis=1, tiled=True),
        "gx",
        split_axis=0,
        concat_axis=0,
        tiled=True,
    )
    return moved


def move_sums(packed):
    moved = lax.all_to_all(
        lax.all_to_all(packed, "gy", split_axis=1, concat_axis=1, tiled=True),
        "gx",
        split_axis=0,
        concat_axis=0,
        tiled=True,
    )
    return moved


def shards(factor, right_sides, send_rows, neighbour_slot):
    blocks = factor.shape[0]
    width = factor.shape[1]
    far_width = factor.shape[2] - width
    senders = send_rows.shape[1]
    capacity = send_rows.shape[2]
    columns = right_sides.shape[1]
    outer = lax.axis_size("gx")
    inner = lax.axis_size("gy")
    places_all = senders * capacity
    rows_here = blocks * width
    tile = 256
    tiled = capacity % 16 == 0 and (inner * capacity) % 128 == 0
    tiled = tiled and inner % 2 == 0 and blocks % 2 == 0 and places_all % tile == 0
    if tiled and width % tile == 0 and far_width % 128 == 0 and columns % 128 == 0:
        return fused(factor, right_sides, send_rows, neighbour_slot, tile)
    outgoing = send_rows.reshape(places_all)
    own_factor = factor[:, :, :width]
    far_factor = factor[:, :, width:]
    place_ids = jnp.arange(places_all, dtype=jnp.int32)
    picker = (neighbour_slot[:, :, None] == place_ids[None, None, :]).astype(jnp.bfloat16)
    spread_factor = jnp.einsum(
        "bij,bjs->bis", far_factor, picker, preferred_element_type=jnp.float32
    ).astype(jnp.bfloat16)
    row_ids = jnp.arange(rows_here, dtype=jnp.int32)
    selector = (outgoing[:, None] == row_ids[None, :]).astype(jnp.bfloat16)
    vector = right_sides
    own_rows = vector.reshape(blocks, width, columns)
    packed = jnp.dot(selector, vector, preferred_element_type=jnp.float32).astype(jnp.bfloat16)
    packed = packed.reshape(outer, inner, capacity, columns)
    received = move_rows(packed).reshape(places_all, columns)
    forward = jnp.einsum("bij,bjr->bir", own_factor, own_rows, preferred_element_type=jnp.float32)
    forward = forward + jnp.einsum(
        "bis,sr->bir", spread_factor, received, preferred_element_type=jnp.float32
    )
    weighted = forward.astype(jnp.bfloat16)
    own_back = jnp.einsum("bij,bir->bjr", own_factor, weighted, preferred_element_type=jnp.float32)
    slot_sums = jnp.einsum(
        "bis,bir->sr", spread_factor, weighted, preferred_element_type=jnp.float32
    )
    slot_sums = slot_sums.astype(jnp.bfloat16).reshape(outer, inner, capacity, columns)
    returned = move_sums(slot_sums).reshape(places_all, columns)
    added = jnp.einsum("sk,sr->kr", selector, returned, preferred_element_type=jnp.float32)
    vector = (own_back.reshape(rows_here, columns) + added).astype(jnp.bfloat16)
    return (weighted.reshape(rows_here, columns), vector)


def solution(mesh):
    in_specs = (
        P(("gx", "gy"), None, None),
        P(("gx", "gy"), None),
        P(("gx", "gy"), None, None),
        P(("gx", "gy"), None),
    )
    out_specs = (P(("gx", "gy"), None), P(("gx", "gy"), None))
    return jax.shard_map(shards, mesh=mesh, in_specs=in_specs, out_specs=out_specs, check_vma=False)
```

```python
import functools

import jax
import jax.numpy as jnp
from jax import lax
from jax.experimental import pallas as pl
from jax.experimental.pallas import tpu as pltpu
from jax.sharding import PartitionSpec as P

MESH = pl.DeviceIdType.MESH
NT = (((1,), (1,)), ((), ()))
TN = (((0,), (0,)), ((), ()))


def one_hot(ids, places):
    one, zero = jnp.bfloat16(1), jnp.bfloat16(0)
    return jnp.where(ids == places, one, zero)


def whole(ids):
    return ids.astype(jnp.float32).astype(jnp.bfloat16)


def within(ids, first, size):
    ids = ids - first
    return whole(jnp.where((ids >= 0) & (ids < size), ids, -1))


def count(n, axis):
    shape = (n, 128) if axis == 0 else (16, n)
    return whole(lax.broadcasted_iota(jnp.int32, shape, axis))


def orders(outer):
    split = outer // 2

    def crosses(a, b):
        return (a < split) != (b < split)

    middle = (outer - 1) / 2
    rows, sums, waits = [], [], []
    for a in range(outer):
        every = range(outer)
        rows.append(sorted(every, key=lambda b: (abs(b - middle), not crosses(a, b), b)))
        near = a == split
        sums.append(
            sorted(every, key=lambda b: (near and not crosses(a, b), near and b == a, abs(b - a) if near else b))
        )
        waits.append(sorted((b for b in every if b != a), key=lambda b: (abs(b - a), b)))
    return rows, sums, waits


def kernel(
    outer, inner, tile,
    factor_ref, vector_ref, table_ref, slots_ref, half, full,
    factor, vector, table, slots, spread_t, picker, packed, received, sums, returned,
    id_rows, id_columns, total_t, half_t, wide,
    load_sem, go_sem, back_go_sem, come_sem, back_come_sem,
):
    blocks, width, _ = factor.shape
    pairs, _ = vector.shape
    columns = half.shape[1]
    senders, capacity, _ = packed.shape
    places = senders * capacity
    span = inner * capacity
    far_width = slots.shape[1]
    side_blocks = blocks // 2
    gx, gy = lax.axis_index("gx"), lax.axis_index("gy")
    me = gx * inner + gy
    row_order, sum_order, wait_order = orders(outer)

    barrier = pltpu.get_barrier_semaphore()

    def greet(k, carry):
        other = lax.rem(me + k, senders)
        pl.semaphore_signal(
            barrier, inc=1, device_id=(other // inner, lax.rem(other, inner)), device_id_type=MESH
        )
        return carry

    loads = [
        pltpu.make_async_copy(table_ref, table, load_sem.at[0]),
        pltpu.make_async_copy(
            vector_ref.at[pl.ds(0, pairs)], vector.at[:, pl.ds(0, columns)], load_sem.at[1]
        ),
        pltpu.make_async_copy(
            vector_ref.at[pl.ds(pairs, pairs)], vector.at[:, pl.ds(columns, columns)], load_sem.at[2]
        ),
        pltpu.make_async_copy(slots_ref, slots, load_sem.at[3]),
        pltpu.make_async_copy(factor_ref, factor, load_sem.at[4]),
    ]
    for load in loads:
        load.start()
    lax.fori_loop(1, senders, greet, 0)

    received[me] = jnp.zeros((capacity, columns), jnp.bfloat16)
    returned[me] = jnp.zeros((capacity, columns), jnp.bfloat16)

    def listed(lists, k):
        plane = jnp.int32(lists[outer - 1][k])
        for i in range(outer - 1):
            plane = jnp.where(gx == i, jnp.int32(lists[i][k]), plane)
        return plane

    def group_places(g):
        return pl.ds(pl.multiple_of(g * span, 128), span)

    def group(ref, g):
        return ref[pl.ds(g * inner, inner)].reshape(span, columns)

    def send_group(source, target, send_sem, recv_sem, plane):
        def step(y, carry):
            to_y = lax.rem(gy + y, inner)
            pltpu.make_async_remote_copy(
                src_ref=source.at[plane * inner + to_y],
                dst_ref=target.at[me],
                send_sem=send_sem,
                recv_sem=recv_sem.at[gx],
                device_id=(plane, to_y),
                device_id_type=MESH,
            ).start()
            return carry

        lax.fori_loop(jnp.where(plane == gx, 1, 0), inner, step, 0)

    def await_bytes(buffer, sem, slabs):
        whole = buffer.at[pl.ds(0, slabs)]
        pltpu.make_async_copy(whole, whole, sem).wait()

    outward = (packed, received, go_sem, come_sem)
    inward = (sums, returned, back_go_sem, back_come_sem)

    loads[0].wait()
    flipped = table[0].T
    for e in range(senders):
        id_columns[pl.ds(e * capacity, capacity), :] = jnp.broadcast_to(
            flipped[:, e : e + 1], (capacity, 128)
        )
    loads[1].wait()
    loads[2].wait()

    def lanes(ids, n):
        return jnp.concatenate([ids] * (n // 128), axis=1)

    def lane_count(n):
        return jnp.concatenate([count(tile, 1)] * (n // 16), axis=0)

    def pack(g):
        part = span // 2
        for r in range(2):
            ids = id_columns[pl.ds(pl.multiple_of(g * span + r * part, 8), part), :]
            upper = ids >= pairs
            ids = jnp.where(upper, ids - pairs, ids)
            rows = jnp.zeros((part, 2 * columns), jnp.float32)
            for c in range(pairs // tile):
                rows = rows + jnp.dot(
                    one_hot(lanes(within(ids, c * tile, tile), tile), lane_count(part)),
                    vector[c * tile : (c + 1) * tile, :],
                    preferred_element_type=jnp.float32,
                )
            upper = lanes(upper.astype(jnp.int32), columns) > 0
            picked = jnp.where(upper, rows[:, columns:], rows[:, :columns])
            packed[pl.ds(g * inner + r * (inner // 2), inner // 2)] = picked.astype(
                jnp.bfloat16
            ).reshape(inner // 2, capacity, columns)

    for k in range(outer):
        plane = listed(row_order, k)
        pack(plane)
        if k == 0:
            pl.semaphore_wait(barrier, senders - 1)
        send_group(*outward, plane)

    loads[3].wait()
    loads[4].wait()

    def rows_of(side, b):
        return pl.ds(pl.multiple_of(b * width, width), width), slice(side * columns, (side + 1) * columns)

    def spread_block(side):
        def step(n, carry):
            b = side * side_blocks + n
            here = pl.ds(pl.multiple_of(b * width, width), width)
            far = factor[b, :, width:]
            ids = slots[pl.ds(b, 1), :]
            for c in range(0, places, 1536):
                hot = [
                    one_hot(
                        jnp.broadcast_to(within(ids, d, tile), (tile, far_width)),
                        lanes(count(tile, 0), far_width),
                    )
                    for d in range(c, c + 1536, tile)
                ]
                spread_t[c : c + 1536, here] = lax.dot_general(
                    jnp.concatenate(hot, axis=0), far, NT, preferred_element_type=jnp.float32
                ).astype(jnp.bfloat16)
            total_t[:, here] = lax.dot_general(
                vector[rows_of(side, n)], factor[b, :, :width], (((0,), (1,)), ((), ())),
                preferred_element_type=jnp.float32,
            )
            return carry

        lax.fori_loop(0, side_blocks, step, 0)

    for side in range(2):
        spread_block(side)

    slab = half.shape[0] // 4
    for n in range(outer):
        if n == 0:
            g = gx
            await_bytes(received, come_sem.at[g], inner - 1)
        else:
            g = listed(wait_order, n - 1)
            await_bytes(received, come_sem.at[g], inner)
        rows_t = group(received, g).T
        for h in range(4):
            part = slice(h * slab, (h + 1) * slab)
            value = total_t[:, part] + jnp.dot(
                rows_t, spread_t[group_places(g), part], preferred_element_type=jnp.float32
            )
            if n < outer - 1:
                total_t[:, part] = value
            else:
                half_t[:, part] = value.astype(jnp.bfloat16)

    for k in range(outer):
        g = listed(sum_order, k)
        value = lax.dot_general(
            spread_t[group_places(g), :], half_t[...], NT, preferred_element_type=jnp.float32
        )
        sums[pl.ds(g * inner, inner)] = value.astype(jnp.bfloat16).reshape(inner, capacity, columns)
        send_group(*inward, g)

    def own_block(side):
        def step(n, carry):
            b = side * side_blocks + n
            here = pl.ds(pl.multiple_of(b * width, width), width)
            wide[rows_of(side, n)] = lax.dot_general(
                factor[b, :, :width], half[here, :], TN, preferred_element_type=jnp.float32
            )
            return carry

        lax.fori_loop(0, side_blocks, step, 0)

    half[...] = half_t[...].T
    for side in range(2):
        own_block(side)
    id_rows[...] = jnp.concatenate([table[0, e : e + 1, :] for e in range(senders)], axis=1)
    id_rows[...] = jnp.where(id_rows[...] >= pairs, id_rows[...] - pairs, id_rows[...])

    def pick_rows(n, carry):
        here = pl.ds(pl.multiple_of(n * width, width), width)
        ids = jnp.broadcast_to(within(id_rows[0:1, :], n * width, width), (width, places))
        picker[here, :] = one_hot(ids, lanes(count(width, 0), places))
        return carry

    lax.fori_loop(0, pairs // width, pick_rows, 0)

    await_bytes(packed, go_sem, senders - 1)

    for n in range(outer):
        if n == 0:
            g = gx
            await_bytes(returned, back_come_sem.at[g], inner - 1)
        else:
            g = listed(wait_order, n - 1)
            await_bytes(returned, back_come_sem.at[g], inner)
        rows = group(returned, g)
        upper = lanes(id_columns[pl.ds(pl.multiple_of(g * span, 8), span), :], columns) >= pairs
        none = jnp.zeros_like(rows)
        both = jnp.concatenate([jnp.where(upper, none, rows), jnp.where(upper, rows, none)], axis=1)
        for h in range(2):
            part = pl.ds(h * (pairs // 2), pairs // 2)
            value = wide[part, :] + jnp.dot(
                picker[part, group_places(g)], both, preferred_element_type=jnp.float32
            )
            if n < outer - 1:
                wide[part, :] = value
            else:
                value = value.astype(jnp.bfloat16)
                full[part, :] = value[:, :columns]
                full[pl.ds(pairs + h * (pairs // 2), pairs // 2), :] = value[:, columns:]
    await_bytes(sums, back_go_sem, senders - 1)


def write_out(half_ref, full_ref, half_out, full_out, sems):
    copies = [
        pltpu.make_async_copy(half_ref, half_out, sems.at[0]),
        pltpu.make_async_copy(full_ref, full_out, sems.at[1]),
    ]
    for copy in copies:
        copy.start()
    for copy in copies:
        copy.wait()


def fused(factor, right_sides, send_rows, neighbour_slot, tile):
    blocks, width, _ = factor.shape
    rows_here, columns = right_sides.shape
    _, senders, capacity = send_rows.shape
    places = senders * capacity
    outer, inner = lax.axis_size("gx"), lax.axis_size("gy")
    kept = jnp.bfloat16
    out = pltpu.VMEM((rows_here, columns), kept)
    moved = pltpu.VMEM((senders, capacity, columns), kept)
    pairs, far_width = rows_here // 2, neighbour_slot.shape[1]
    flag, flags = pltpu.SemaphoreType.DMA, pltpu.SemaphoreType.DMA((outer,))
    half, full = pl.pallas_call(
        functools.partial(kernel, outer, inner, tile),
        out_shape=(out, out),
        in_specs=[pl.BlockSpec(memory_space=pl.ANY)] * 4,
        out_specs=(pl.BlockSpec(memory_space=pltpu.VMEM),) * 2,
        scratch_shapes=[
            pltpu.VMEM(factor.shape, kept),
            pltpu.VMEM((pairs, 2 * columns), kept),
            pltpu.VMEM(send_rows.shape, jnp.int32),
            pltpu.VMEM(neighbour_slot.shape, jnp.int32),
            pltpu.VMEM((places, rows_here), kept),
            pltpu.VMEM((pairs, places), kept),
            moved, moved, moved, moved,
            pltpu.VMEM((1, places), jnp.int32),
            pltpu.VMEM((places, 128), jnp.int32),
            pltpu.VMEM((columns, rows_here), jnp.float32),
            pltpu.VMEM((columns, rows_here), kept),
            pltpu.VMEM((pairs, 2 * columns), jnp.float32),
            pltpu.SemaphoreType.DMA((5,)),
            flag, flag, flags, flags,
        ],
        compiler_params=pltpu.CompilerParams(collective_id=0, has_side_effects=True),
    )(factor, right_sides, send_rows, neighbour_slot)
    written = jax.ShapeDtypeStruct((rows_here, columns), kept)
    return pl.pallas_call(
        write_out,
        out_shape=(written, written),
        in_specs=[pl.BlockSpec(memory_space=pltpu.VMEM)] * 2,
        out_specs=(pl.BlockSpec(memory_space=pl.ANY),) * 2,
        scratch_shapes=[pltpu.SemaphoreType.DMA((2,))],
        compiler_params=pltpu.CompilerParams(vmem_limit_bytes=1 << 20),
    )(half, full)


def move_rows(packed):
    moved = lax.all_to_all(
        lax.all_to_all(packed, "gy", split_axis=1, concat_axis=1, tiled=True),
        "gx",
        split_axis=0,
        concat_axis=0,
        tiled=True,
    )
    return moved


def move_sums(packed):
    moved = lax.all_to_all(
        lax.all_to_all(packed, "gy", split_axis=1, concat_axis=1, tiled=True),
        "gx",
        split_axis=0,
        concat_axis=0,
        tiled=True,
    )
    return moved


def shards(factor, right_sides, send_rows, neighbour_slot):
    blocks = factor.shape[0]
    width = factor.shape[1]
    far_width = factor.shape[2] - width
    senders = send_rows.shape[1]
    capacity = send_rows.shape[2]
    columns = right_sides.shape[1]
    outer = lax.axis_size("gx")
    inner = lax.axis_size("gy")
    places_all = senders * capacity
    rows_here = blocks * width
    tile = 256
    tiled = capacity % 16 == 0 and (inner * capacity) % 128 == 0
    tiled = tiled and inner % 2 == 0 and blocks % 2 == 0 and places_all % tile == 0
    if tiled and width % tile == 0 and far_width % 128 == 0 and columns % 128 == 0:
        return fused(factor, right_sides, send_rows, neighbour_slot, tile)
    outgoing = send_rows.reshape(places_all)
    own_factor = factor[:, :, :width]
    far_factor = factor[:, :, width:]
    place_ids = jnp.arange(places_all, dtype=jnp.int32)
    picker = (neighbour_slot[:, :, None] == place_ids[None, None, :]).astype(jnp.bfloat16)
    spread_factor = jnp.einsum(
        "bij,bjs->bis", far_factor, picker, preferred_element_type=jnp.float32
    ).astype(jnp.bfloat16)
    row_ids = jnp.arange(rows_here, dtype=jnp.int32)
    selector = (outgoing[:, None] == row_ids[None, :]).astype(jnp.bfloat16)
    vector = right_sides
    own_rows = vector.reshape(blocks, width, columns)
    packed = jnp.dot(selector, vector, preferred_element_type=jnp.float32).astype(jnp.bfloat16)
    packed = packed.reshape(outer, inner, capacity, columns)
    received = move_rows(packed).reshape(places_all, columns)
    forward = jnp.einsum("bij,bjr->bir", own_factor, own_rows, preferred_element_type=jnp.float32)
    forward = forward + jnp.einsum(
        "bis,sr->bir", spread_factor, received, preferred_element_type=jnp.float32
    )
    weighted = forward.astype(jnp.bfloat16)
    own_back = jnp.einsum("bij,bir->bjr", own_factor, weighted, preferred_element_type=jnp.float32)
    slot_sums = jnp.einsum(
        "bis,bir->sr", spread_factor, weighted, preferred_element_type=jnp.float32
    )
    slot_sums = slot_sums.astype(jnp.bfloat16).reshape(outer, inner, capacity, columns)
    returned = move_sums(slot_sums).reshape(places_all, columns)
    added = jnp.einsum("sk,sr->kr", selector, returned, preferred_element_type=jnp.float32)
    vector = (own_back.reshape(rows_here, columns) + added).astype(jnp.bfloat16)
    return (weighted.reshape(rows_here, columns), vector)


def solution(mesh):
    in_specs = (
        P(("gx", "gy"), None, None),
        P(("gx", "gy"), None),
        P(("gx", "gy"), None, None),
        P(("gx", "gy"), None),
    )
    out_specs = (P(("gx", "gy"), None), P(("gx", "gy"), None))
    return jax.shard_map(shards, mesh=mesh, in_specs=in_specs, out_specs=out_specs, check_vma=False)
```

```python
import functools

import jax
import jax.numpy as jnp
from jax import lax
from jax.experimental import pallas as pl
from jax.experimental.pallas import tpu as pltpu
from jax.sharding import PartitionSpec as P

MESH = pl.DeviceIdType.MESH
NT = (((1,), (1,)), ((), ()))
TN = (((0,), (0,)), ((), ()))


def one_hot(ids, places):
    one, zero = jnp.bfloat16(1), jnp.bfloat16(0)
    return jnp.where(ids == places, one, zero)


def whole(ids):
    return ids.astype(jnp.float32).astype(jnp.bfloat16)


def within(ids, first, size):
    ids = ids - first
    return whole(jnp.where((ids >= 0) & (ids < size), ids, -1))


def count(n, axis):
    shape = (n, 128) if axis == 0 else (16, n)
    return whole(lax.broadcasted_iota(jnp.int32, shape, axis))


def orders(outer):
    split = outer // 2

    def crosses(a, b):
        return (a < split) != (b < split)

    middle, last = (outer - 1) / 2, outer - 1
    rows, sums, waits = [], [], []
    for a in range(outer):
        every = range(outer)
        aside = split <= a < last
        rows.append(
            sorted(
                every,
                key=lambda b: (b == last, aside or abs(b - middle), not crosses(a, b), abs(b - a) if aside else b),
            )
        )
        sums.append(sorted(every, key=lambda b: (b >= split, b if b < split or a == split - 1 else -b)))
        waits.append(sorted((b for b in every if b != a), key=lambda b: (abs(b - a), b)))
    return rows, sums, waits


def kernel(
    outer, inner, tile,
    factor_ref, vector_ref, table_ref, slots_ref, half, full,
    factor, vector, table, slots, spread_t, picker, packed, received, sums, returned,
    id_rows, id_columns, total_t, half_t, wide,
    load_sem, late_sem, go_sem, back_go_sem, come_sem, back_come_sem,
):
    blocks, width, _ = factor.shape
    pairs, _ = vector.shape
    columns = half.shape[1]
    senders, capacity, _ = packed.shape
    places = senders * capacity
    span = inner * capacity
    far_width = slots.shape[1]
    side_blocks = blocks // 2
    gx, gy = lax.axis_index("gx"), lax.axis_index("gy")
    me = gx * inner + gy
    row_order, sum_order, wait_order = orders(outer)

    barrier = pltpu.get_barrier_semaphore()

    def greet(k, carry):
        other = lax.rem(me + k, senders)
        pl.semaphore_signal(
            barrier, inc=1, device_id=(other // inner, lax.rem(other, inner)), device_id_type=MESH
        )
        return carry

    loads = [
        pltpu.make_async_copy(table_ref, table, load_sem.at[0]),
        pltpu.make_async_copy(
            vector_ref.at[pl.ds(0, pairs)], vector.at[:, pl.ds(0, columns)], load_sem.at[1]
        ),
        pltpu.make_async_copy(
            vector_ref.at[pl.ds(pairs, pairs)], vector.at[:, pl.ds(columns, columns)], load_sem.at[2]
        ),
        pltpu.make_async_copy(slots_ref, slots, load_sem.at[3]),
        pltpu.make_async_copy(factor_ref, factor, load_sem.at[4]),
    ]
    for load in loads:
        load.start()
    last = outer - 1
    early = last * inner
    is_last = gx == last
    lax.fori_loop(1, jnp.where(is_last, 1, senders), greet, 0)

    def greet_plane(y, carry):
        pl.semaphore_signal(
            barrier, inc=1, device_id=(gx, lax.rem(gy + y, inner)), device_id_type=MESH
        )
        return carry

    lax.fori_loop(1, jnp.where(is_last, inner, 1), greet_plane, 0)

    def announce(k, carry):
        pl.semaphore_signal(
            late_sem, inc=1, device_id=(k // inner, lax.rem(k, inner)), device_id_type=MESH
        )
        return carry

    def meet():
        @pl.when(is_last)
        def _():
            pl.semaphore_wait(barrier, senders - 1)
            lax.fori_loop(0, early, announce, 0)

        @pl.when(jnp.logical_not(is_last))
        def _():
            pl.semaphore_wait(barrier, early - 1)

    received[me] = jnp.zeros((capacity, columns), jnp.bfloat16)
    returned[me] = jnp.zeros((capacity, columns), jnp.bfloat16)

    def listed(lists, k):
        plane = jnp.int32(lists[outer - 1][k])
        for i in range(outer - 1):
            plane = jnp.where(gx == i, jnp.int32(lists[i][k]), plane)
        return plane

    def group_places(g):
        return pl.ds(pl.multiple_of(g * span, 128), span)

    def group(ref, g):
        return ref[pl.ds(g * inner, inner)].reshape(span, columns)

    def send_group(source, target, send_sem, recv_sem, plane):
        def send(y):
            to_y = lax.rem(gy + y, inner)
            pltpu.make_async_remote_copy(
                src_ref=source.at[plane * inner + to_y],
                dst_ref=target.at[me],
                send_sem=send_sem,
                recv_sem=recv_sem.at[gx],
                device_id=(plane, to_y),
                device_id_type=MESH,
            ).start()

        for y in range(1, inner):
            send(y)

        @pl.when(plane != gx)
        def _():
            send(0)

    def await_bytes(buffer, sem, slabs):
        whole = buffer.at[pl.ds(0, slabs)]
        pltpu.make_async_copy(whole, whole, sem).wait()

    outward = (packed, received, go_sem, come_sem)
    inward = (sums, returned, back_go_sem, back_come_sem)

    loads[0].wait()
    flipped = table[0].T
    for e in range(senders):
        id_columns[pl.ds(e * capacity, capacity), :] = jnp.broadcast_to(
            flipped[:, e : e + 1], (capacity, 128)
        )
    loads[1].wait()
    loads[2].wait()

    def lanes(ids, n):
        return jnp.concatenate([ids] * (n // 128), axis=1)

    def lane_count(n):
        return jnp.concatenate([count(tile, 1)] * (n // 16), axis=0)

    def pack(g):
        part = span // 2
        for r in range(2):
            ids = id_columns[pl.ds(pl.multiple_of(g * span + r * part, 8), part), :]
            upper = ids >= pairs
            ids = jnp.where(upper, ids - pairs, ids)
            rows = jnp.zeros((part, 2 * columns), jnp.float32)
            for c in range(pairs // tile):
                rows = rows + jnp.dot(
                    one_hot(lanes(within(ids, c * tile, tile), tile), lane_count(part)),
                    vector[c * tile : (c + 1) * tile, :],
                    preferred_element_type=jnp.float32,
                )
            upper = lanes(upper.astype(jnp.int32), columns) > 0
            picked = jnp.where(upper, rows[:, columns:], rows[:, :columns])
            packed[pl.ds(g * inner + r * (inner // 2), inner // 2)] = picked.astype(
                jnp.bfloat16
            ).reshape(inner // 2, capacity, columns)

    for k in range(outer):
        plane = listed(row_order, k)
        pack(plane)
        if k == 0:
            meet()

        @pl.when((plane == last) & jnp.logical_not(is_last))
        def _():
            pl.semaphore_wait(late_sem, inner)

        send_group(*outward, plane)

    loads[3].wait()
    loads[4].wait()

    def rows_of(side, b):
        return pl.ds(pl.multiple_of(b * width, width), width), slice(side * columns, (side + 1) * columns)

    def spread_block(side):
        def step(n, carry):
            b = side * side_blocks + n
            here = pl.ds(pl.multiple_of(b * width, width), width)
            far = factor[b, :, width:]
            ids = slots[pl.ds(b, 1), :]
            for c in range(0, places, 1536):
                hot = [
                    one_hot(
                        jnp.broadcast_to(within(ids, d, tile), (tile, far_width)),
                        lanes(count(tile, 0), far_width),
                    )
                    for d in range(c, c + 1536, tile)
                ]
                spread_t[c : c + 1536, here] = lax.dot_general(
                    jnp.concatenate(hot, axis=0), far, NT, preferred_element_type=jnp.float32
                ).astype(jnp.bfloat16)
            total_t[:, here] = lax.dot_general(
                vector[rows_of(side, n)], factor[b, :, :width], (((0,), (1,)), ((), ())),
                preferred_element_type=jnp.float32,
            )
            return carry

        lax.fori_loop(0, side_blocks, step, 0)

    for side in range(2):
        spread_block(side)

    slab = half.shape[0] // 4
    for n in range(outer):
        if n == 0:
            g = gx
            await_bytes(received, come_sem.at[g], inner - 1)
        else:
            g = listed(wait_order, n - 1)
            await_bytes(received, come_sem.at[g], inner)
        rows_t = group(received, g).T
        for h in range(4):
            part = slice(h * slab, (h + 1) * slab)
            value = total_t[:, part] + jnp.dot(
                rows_t, spread_t[group_places(g), part], preferred_element_type=jnp.float32
            )
            if n < outer - 1:
                total_t[:, part] = value
            else:
                half_t[:, part] = value.astype(jnp.bfloat16)

    for k in range(outer):
        g = listed(sum_order, k)
        value = lax.dot_general(
            spread_t[group_places(g), :], half_t[...], NT, preferred_element_type=jnp.float32
        )
        sums[pl.ds(g * inner, inner)] = value.astype(jnp.bfloat16).reshape(inner, capacity, columns)
        send_group(*inward, g)

    def own_block(side):
        def step(n, carry):
            b = side * side_blocks + n
            here = pl.ds(pl.multiple_of(b * width, width), width)
            wide[rows_of(side, n)] = lax.dot_general(
                factor[b, :, :width], half[here, :], TN, preferred_element_type=jnp.float32
            )
            return carry

        lax.fori_loop(0, side_blocks, step, 0)

    half[...] = half_t[...].T
    for side in range(2):
        own_block(side)
    id_rows[...] = jnp.concatenate([table[0, e : e + 1, :] for e in range(senders)], axis=1)
    id_rows[...] = jnp.where(id_rows[...] >= pairs, id_rows[...] - pairs, id_rows[...])

    def pick_rows(n, carry):
        here = pl.ds(pl.multiple_of(n * width, width), width)
        ids = jnp.broadcast_to(within(id_rows[0:1, :], n * width, width), (width, places))
        picker[here, :] = one_hot(ids, lanes(count(width, 0), places))
        return carry

    lax.fori_loop(0, pairs // width, pick_rows, 0)

    await_bytes(packed, go_sem, senders - 1)

    for n in range(outer):
        if n == 0:
            g = gx
            await_bytes(returned, back_come_sem.at[g], inner - 1)
        else:
            g = listed(wait_order, n - 1)
            await_bytes(returned, back_come_sem.at[g], inner)
        rows = group(returned, g)
        upper = lanes(id_columns[pl.ds(pl.multiple_of(g * span, 8), span), :], columns) >= pairs
        none = jnp.zeros_like(rows)
        both = jnp.concatenate([jnp.where(upper, none, rows), jnp.where(upper, rows, none)], axis=1)
        for h in range(2):
            part = pl.ds(h * (pairs // 2), pairs // 2)
            value = wide[part, :] + jnp.dot(
                picker[part, group_places(g)], both, preferred_element_type=jnp.float32
            )
            if n < outer - 1:
                wide[part, :] = value
            else:
                value = value.astype(jnp.bfloat16)
                full[part, :] = value[:, :columns]
                full[pl.ds(pairs + h * (pairs // 2), pairs // 2), :] = value[:, columns:]
    await_bytes(sums, back_go_sem, senders - 1)


def write_out(half_ref, full_ref, half_out, full_out, sems):
    copies = [
        pltpu.make_async_copy(half_ref, half_out, sems.at[0]),
        pltpu.make_async_copy(full_ref, full_out, sems.at[1]),
    ]
    for copy in copies:
        copy.start()
    for copy in copies:
        copy.wait()


def fused(factor, right_sides, send_rows, neighbour_slot, tile):
    blocks, width, _ = factor.shape
    rows_here, columns = right_sides.shape
    _, senders, capacity = send_rows.shape
    places = senders * capacity
    outer, inner = lax.axis_size("gx"), lax.axis_size("gy")
    kept = jnp.bfloat16
    out = pltpu.VMEM((rows_here, columns), kept)
    moved = pltpu.VMEM((senders, capacity, columns), kept)
    pairs, far_width = rows_here // 2, neighbour_slot.shape[1]
    flag, flags = pltpu.SemaphoreType.DMA, pltpu.SemaphoreType.DMA((outer,))
    half, full = pl.pallas_call(
        functools.partial(kernel, outer, inner, tile),
        out_shape=(out, out),
        in_specs=[pl.BlockSpec(memory_space=pl.ANY)] * 4,
        out_specs=(pl.BlockSpec(memory_space=pltpu.VMEM),) * 2,
        scratch_shapes=[
            pltpu.VMEM(factor.shape, kept),
            pltpu.VMEM((pairs, 2 * columns), kept),
            pltpu.VMEM(send_rows.shape, jnp.int32),
            pltpu.VMEM(neighbour_slot.shape, jnp.int32),
            pltpu.VMEM((places, rows_here), kept),
            pltpu.VMEM((pairs, places), kept),
            moved, moved, moved, moved,
            pltpu.VMEM((1, places), jnp.int32),
            pltpu.VMEM((places, 128), jnp.int32),
            pltpu.VMEM((columns, rows_here), jnp.float32),
            pltpu.VMEM((columns, rows_here), kept),
            pltpu.VMEM((pairs, 2 * columns), jnp.float32),
            pltpu.SemaphoreType.DMA((5,)),
            pltpu.SemaphoreType.REGULAR,
            flag, flag, flags, flags,
        ],
        compiler_params=pltpu.CompilerParams(collective_id=0, has_side_effects=True),
    )(factor, right_sides, send_rows, neighbour_slot)
    written = jax.ShapeDtypeStruct((rows_here, columns), kept)
    return pl.pallas_call(
        write_out,
        out_shape=(written, written),
        in_specs=[pl.BlockSpec(memory_space=pltpu.VMEM)] * 2,
        out_specs=(pl.BlockSpec(memory_space=pl.ANY),) * 2,
        scratch_shapes=[pltpu.SemaphoreType.DMA((2,))],
        compiler_params=pltpu.CompilerParams(vmem_limit_bytes=1 << 20),
    )(half, full)


def move_rows(packed):
    moved = lax.all_to_all(
        lax.all_to_all(packed, "gy", split_axis=1, concat_axis=1, tiled=True),
        "gx",
        split_axis=0,
        concat_axis=0,
        tiled=True,
    )
    return moved


def move_sums(packed):
    moved = lax.all_to_all(
        lax.all_to_all(packed, "gy", split_axis=1, concat_axis=1, tiled=True),
        "gx",
        split_axis=0,
        concat_axis=0,
        tiled=True,
    )
    return moved


def shards(factor, right_sides, send_rows, neighbour_slot):
    blocks = factor.shape[0]
    width = factor.shape[1]
    far_width = factor.shape[2] - width
    senders = send_rows.shape[1]
    capacity = send_rows.shape[2]
    columns = right_sides.shape[1]
    outer = lax.axis_size("gx")
    inner = lax.axis_size("gy")
    places_all = senders * capacity
    rows_here = blocks * width
    tile = 256
    tiled = capacity % 16 == 0 and (inner * capacity) % 128 == 0
    tiled = tiled and outer > 1 and inner % 2 == 0 and blocks % 2 == 0 and places_all % tile == 0
    if tiled and width % tile == 0 and far_width % 128 == 0 and columns % 128 == 0:
        return fused(factor, right_sides, send_rows, neighbour_slot, tile)
    outgoing = send_rows.reshape(places_all)
    own_factor = factor[:, :, :width]
    far_factor = factor[:, :, width:]
    place_ids = jnp.arange(places_all, dtype=jnp.int32)
    picker = (neighbour_slot[:, :, None] == place_ids[None, None, :]).astype(jnp.bfloat16)
    spread_factor = jnp.einsum(
        "bij,bjs->bis", far_factor, picker, preferred_element_type=jnp.float32
    ).astype(jnp.bfloat16)
    row_ids = jnp.arange(rows_here, dtype=jnp.int32)
    selector = (outgoing[:, None] == row_ids[None, :]).astype(jnp.bfloat16)
    vector = right_sides
    own_rows = vector.reshape(blocks, width, columns)
    packed = jnp.dot(selector, vector, preferred_element_type=jnp.float32).astype(jnp.bfloat16)
    packed = packed.reshape(outer, inner, capacity, columns)
    received = move_rows(packed).reshape(places_all, columns)
    forward = jnp.einsum("bij,bjr->bir", own_factor, own_rows, preferred_element_type=jnp.float32)
    forward = forward + jnp.einsum(
        "bis,sr->bir", spread_factor, received, preferred_element_type=jnp.float32
    )
    weighted = forward.astype(jnp.bfloat16)
    own_back = jnp.einsum("bij,bir->bjr", own_factor, weighted, preferred_element_type=jnp.float32)
    slot_sums = jnp.einsum(
        "bis,bir->sr", spread_factor, weighted, preferred_element_type=jnp.float32
    )
    slot_sums = slot_sums.astype(jnp.bfloat16).reshape(outer, inner, capacity, columns)
    returned = move_sums(slot_sums).reshape(places_all, columns)
    added = jnp.einsum("sk,sr->kr", selector, returned, preferred_element_type=jnp.float32)
    vector = (own_back.reshape(rows_here, columns) + added).astype(jnp.bfloat16)
    return (weighted.reshape(rows_here, columns), vector)


def solution(mesh):
    in_specs = (
        P(("gx", "gy"), None, None),
        P(("gx", "gy"), None),
        P(("gx", "gy"), None, None),
        P(("gx", "gy"), None),
    )
    out_specs = (P(("gx", "gy"), None), P(("gx", "gy"), None))
    return jax.shard_map(shards, mesh=mesh, in_specs=in_specs, out_specs=out_specs, check_vma=False)
```

```python
import functools

import jax
import jax.numpy as jnp
from jax import lax
from jax.experimental import pallas as pl
from jax.experimental.pallas import tpu as pltpu
from jax.sharding import PartitionSpec as P

MESH = pl.DeviceIdType.MESH
NT = (((1,), (1,)), ((), ()))
TN = (((0,), (0,)), ((), ()))


def one_hot(ids, places):
    one, zero = jnp.bfloat16(1), jnp.bfloat16(0)
    return jnp.where(ids == places, one, zero)


def whole(ids):
    return ids.astype(jnp.float32).astype(jnp.bfloat16)


def within(ids, first, size):
    ids = ids - first
    return whole(jnp.where((ids >= 0) & (ids < size), ids, -1))


def count(n, axis):
    shape = (n, 128) if axis == 0 else (16, n)
    return whole(lax.broadcasted_iota(jnp.int32, shape, axis))


def orders(outer):
    split = outer // 2

    def crosses(a, b):
        return (a < split) != (b < split)

    middle, last = (outer - 1) / 2, outer - 1
    rows, sums, waits = [], [], []
    for a in range(outer):
        every = range(outer)
        aside = split <= a < last
        rows.append(
            sorted(
                every,
                key=lambda b: (b == last, aside or abs(b - middle), not crosses(a, b), abs(b - a) if aside else b),
            )
        )
        sums.append(sorted(every, key=lambda b: (b >= split, b if b < split or a in (split - 1, last) else -b)))
        waits.append(sorted((b for b in every if b != a), key=lambda b: (abs(b - a), b)))
    return rows, sums, waits


def kernel(
    outer, inner, tile,
    factor_ref, vector_ref, table_ref, slots_ref, half, full,
    factor, vector, table, slots, spread_t, picker, packed, received, sums, returned,
    id_rows, id_columns, total_t, half_t, wide,
    load_sem, late_sem, go_sem, back_go_sem, come_sem, back_come_sem,
):
    blocks, width, _ = factor.shape
    pairs, _ = vector.shape
    columns = half.shape[1]
    senders, capacity, _ = packed.shape
    places = senders * capacity
    span = inner * capacity
    far_width = slots.shape[1]
    side_blocks = blocks // 2
    gx, gy = lax.axis_index("gx"), lax.axis_index("gy")
    me = gx * inner + gy
    row_order, sum_order, wait_order = orders(outer)

    barrier = pltpu.get_barrier_semaphore()

    def greet(k, carry):
        other = lax.rem(me + k, senders)
        pl.semaphore_signal(
            barrier, inc=1, device_id=(other // inner, lax.rem(other, inner)), device_id_type=MESH
        )
        return carry

    loads = [
        pltpu.make_async_copy(table_ref, table, load_sem.at[0]),
        pltpu.make_async_copy(
            vector_ref.at[pl.ds(0, pairs)], vector.at[:, pl.ds(0, columns)], load_sem.at[1]
        ),
        pltpu.make_async_copy(
            vector_ref.at[pl.ds(pairs, pairs)], vector.at[:, pl.ds(columns, columns)], load_sem.at[2]
        ),
        pltpu.make_async_copy(slots_ref, slots, load_sem.at[3]),
        pltpu.make_async_copy(factor_ref, factor, load_sem.at[4]),
    ]
    for load in loads:
        load.start()
    last = outer - 1
    early = last * inner
    is_last = gx == last
    lax.fori_loop(1, jnp.where(is_last, 1, senders), greet, 0)

    def greet_plane(y, carry):
        pl.semaphore_signal(
            barrier, inc=1, device_id=(gx, lax.rem(gy + y, inner)), device_id_type=MESH
        )
        return carry

    lax.fori_loop(1, jnp.where(is_last, inner, 1), greet_plane, 0)

    def announce(k, carry):
        pl.semaphore_signal(
            late_sem, inc=1, device_id=(k // inner, lax.rem(k, inner)), device_id_type=MESH
        )
        return carry

    def meet():
        @pl.when(is_last)
        def _():
            pl.semaphore_wait(barrier, senders - 1)
            lax.fori_loop(0, early, announce, 0)

        @pl.when(jnp.logical_not(is_last))
        def _():
            pl.semaphore_wait(barrier, early - 1)

    received[me] = jnp.zeros((capacity, columns), jnp.bfloat16)
    returned[me] = jnp.zeros((capacity, columns), jnp.bfloat16)

    def listed(lists, k):
        plane = jnp.int32(lists[outer - 1][k])
        for i in range(outer - 1):
            plane = jnp.where(gx == i, jnp.int32(lists[i][k]), plane)
        return plane

    def group_places(g):
        return pl.ds(pl.multiple_of(g * span, 128), span)

    def group(ref, g):
        return ref[pl.ds(g * inner, inner)].reshape(span, columns)

    def send_group(source, target, send_sem, recv_sem, plane):
        def send(y):
            to_y = lax.rem(gy + inner - y, inner)
            pltpu.make_async_remote_copy(
                src_ref=source.at[plane * inner + to_y],
                dst_ref=target.at[me],
                send_sem=send_sem,
                recv_sem=recv_sem.at[gx],
                device_id=(plane, to_y),
                device_id_type=MESH,
            ).start()

        for y in range(1, inner):
            send(y)

        @pl.when(plane != gx)
        def _():
            send(0)

    def await_bytes(buffer, sem, slabs):
        whole = buffer.at[pl.ds(0, slabs)]
        pltpu.make_async_copy(whole, whole, sem).wait()

    outward = (packed, received, go_sem, come_sem)
    inward = (sums, returned, back_go_sem, back_come_sem)

    loads[0].wait()
    flipped = table[0].T
    for e in range(senders):
        id_columns[pl.ds(e * capacity, capacity), :] = jnp.broadcast_to(
            flipped[:, e : e + 1], (capacity, 128)
        )
    loads[1].wait()
    loads[2].wait()

    def lanes(ids, n):
        return jnp.concatenate([ids] * (n // 128), axis=1)

    def lane_count(n):
        return jnp.concatenate([count(tile, 1)] * (n // 16), axis=0)

    def pack(g):
        part = span // 2
        for r in range(2):
            ids = id_columns[pl.ds(pl.multiple_of(g * span + r * part, 8), part), :]
            upper = ids >= pairs
            ids = jnp.where(upper, ids - pairs, ids)
            rows = jnp.zeros((part, 2 * columns), jnp.float32)
            for c in range(pairs // tile):
                rows = rows + jnp.dot(
                    one_hot(lanes(within(ids, c * tile, tile), tile), lane_count(part)),
                    vector[c * tile : (c + 1) * tile, :],
                    preferred_element_type=jnp.float32,
                )
            upper = lanes(upper.astype(jnp.int32), columns) > 0
            picked = jnp.where(upper, rows[:, columns:], rows[:, :columns])
            packed[pl.ds(g * inner + r * (inner // 2), inner // 2)] = picked.astype(
                jnp.bfloat16
            ).reshape(inner // 2, capacity, columns)

    for k in range(outer):
        plane = listed(row_order, k)
        pack(plane)
        if k == 0:
            meet()

        @pl.when((plane == last) & jnp.logical_not(is_last))
        def _():
            pl.semaphore_wait(late_sem, inner)

        send_group(*outward, plane)

    loads[3].wait()
    loads[4].wait()

    def rows_of(side, b):
        return pl.ds(pl.multiple_of(b * width, width), width), slice(side * columns, (side + 1) * columns)

    def spread_block(side):
        def step(n, carry):
            b = side * side_blocks + n
            here = pl.ds(pl.multiple_of(b * width, width), width)
            far = factor[b, :, width:]
            ids = slots[pl.ds(b, 1), :]
            for c in range(0, places, 1536):
                hot = [
                    one_hot(
                        jnp.broadcast_to(within(ids, d, tile), (tile, far_width)),
                        lanes(count(tile, 0), far_width),
                    )
                    for d in range(c, c + 1536, tile)
                ]
                spread_t[c : c + 1536, here] = lax.dot_general(
                    jnp.concatenate(hot, axis=0), far, NT, preferred_element_type=jnp.float32
                ).astype(jnp.bfloat16)
            total_t[:, here] = lax.dot_general(
                vector[rows_of(side, n)], factor[b, :, :width], (((0,), (1,)), ((), ())),
                preferred_element_type=jnp.float32,
            )
            return carry

        lax.fori_loop(0, side_blocks, step, 0)

    for side in range(2):
        spread_block(side)

    slab = half.shape[0] // 4
    for n in range(outer):
        if n == 0:
            g = gx
            await_bytes(received, come_sem.at[g], inner - 1)
        else:
            g = listed(wait_order, n - 1)
            await_bytes(received, come_sem.at[g], inner)
        rows_t = group(received, g).T
        for h in range(4):
            part = slice(h * slab, (h + 1) * slab)
            value = total_t[:, part] + jnp.dot(
                rows_t, spread_t[group_places(g), part], preferred_element_type=jnp.float32
            )
            if n < outer - 1:
                total_t[:, part] = value
            else:
                half_t[:, part] = value.astype(jnp.bfloat16)

    for k in range(outer):
        g = listed(sum_order, k)
        value = lax.dot_general(
            spread_t[group_places(g), :], half_t[...], NT, preferred_element_type=jnp.float32
        )
        sums[pl.ds(g * inner, inner)] = value.astype(jnp.bfloat16).reshape(inner, capacity, columns)
        send_group(*inward, g)

    def own_block(side):
        def step(n, carry):
            b = side * side_blocks + n
            here = pl.ds(pl.multiple_of(b * width, width), width)
            wide[rows_of(side, n)] = lax.dot_general(
                factor[b, :, :width], half[here, :], TN, preferred_element_type=jnp.float32
            )
            return carry

        lax.fori_loop(0, side_blocks, step, 0)

    half[...] = half_t[...].T
    for side in range(2):
        own_block(side)
    id_rows[...] = jnp.concatenate([table[0, e : e + 1, :] for e in range(senders)], axis=1)
    id_rows[...] = jnp.where(id_rows[...] >= pairs, id_rows[...] - pairs, id_rows[...])

    def pick_rows(n, carry):
        here = pl.ds(pl.multiple_of(n * width, width), width)
        ids = jnp.broadcast_to(within(id_rows[0:1, :], n * width, width), (width, places))
        picker[here, :] = one_hot(ids, lanes(count(width, 0), places))
        return carry

    lax.fori_loop(0, pairs // width, pick_rows, 0)

    await_bytes(packed, go_sem, senders - 1)

    for n in range(outer):
        if n == 0:
            g = gx
            await_bytes(returned, back_come_sem.at[g], inner - 1)
        else:
            g = listed(wait_order, n - 1)
            await_bytes(returned, back_come_sem.at[g], inner)
        rows = group(returned, g)
        upper = lanes(id_columns[pl.ds(pl.multiple_of(g * span, 8), span), :], columns) >= pairs
        none = jnp.zeros_like(rows)
        both = jnp.concatenate([jnp.where(upper, none, rows), jnp.where(upper, rows, none)], axis=1)
        for h in range(2):
            part = pl.ds(h * (pairs // 2), pairs // 2)
            value = wide[part, :] + jnp.dot(
                picker[part, group_places(g)], both, preferred_element_type=jnp.float32
            )
            if n < outer - 1:
                wide[part, :] = value
            else:
                value = value.astype(jnp.bfloat16)
                full[part, :] = value[:, :columns]
                full[pl.ds(pairs + h * (pairs // 2), pairs // 2), :] = value[:, columns:]
    await_bytes(sums, back_go_sem, senders - 1)


def write_out(half_ref, full_ref, half_out, full_out, sems):
    copies = [
        pltpu.make_async_copy(half_ref, half_out, sems.at[0]),
        pltpu.make_async_copy(full_ref, full_out, sems.at[1]),
    ]
    for copy in copies:
        copy.start()
    for copy in copies:
        copy.wait()


def fused(factor, right_sides, send_rows, neighbour_slot, tile):
    blocks, width, _ = factor.shape
    rows_here, columns = right_sides.shape
    _, senders, capacity = send_rows.shape
    places = senders * capacity
    outer, inner = lax.axis_size("gx"), lax.axis_size("gy")
    kept = jnp.bfloat16
    out = pltpu.VMEM((rows_here, columns), kept)
    moved = pltpu.VMEM((senders, capacity, columns), kept)
    pairs, far_width = rows_here // 2, neighbour_slot.shape[1]
    flag, flags = pltpu.SemaphoreType.DMA, pltpu.SemaphoreType.DMA((outer,))
    half, full = pl.pallas_call(
        functools.partial(kernel, outer, inner, tile),
        out_shape=(out, out),
        in_specs=[pl.BlockSpec(memory_space=pl.ANY)] * 4,
        out_specs=(pl.BlockSpec(memory_space=pltpu.VMEM),) * 2,
        scratch_shapes=[
            pltpu.VMEM(factor.shape, kept),
            pltpu.VMEM((pairs, 2 * columns), kept),
            pltpu.VMEM(send_rows.shape, jnp.int32),
            pltpu.VMEM(neighbour_slot.shape, jnp.int32),
            pltpu.VMEM((places, rows_here), kept),
            pltpu.VMEM((pairs, places), kept),
            moved, moved, moved, moved,
            pltpu.VMEM((1, places), jnp.int32),
            pltpu.VMEM((places, 128), jnp.int32),
            pltpu.VMEM((columns, rows_here), jnp.float32),
            pltpu.VMEM((columns, rows_here), kept),
            pltpu.VMEM((pairs, 2 * columns), jnp.float32),
            pltpu.SemaphoreType.DMA((5,)),
            pltpu.SemaphoreType.REGULAR,
            flag, flag, flags, flags,
        ],
        compiler_params=pltpu.CompilerParams(collective_id=0, has_side_effects=True),
    )(factor, right_sides, send_rows, neighbour_slot)
    written = jax.ShapeDtypeStruct((rows_here, columns), kept)
    return pl.pallas_call(
        write_out,
        out_shape=(written, written),
        in_specs=[pl.BlockSpec(memory_space=pltpu.VMEM)] * 2,
        out_specs=(pl.BlockSpec(memory_space=pl.ANY),) * 2,
        scratch_shapes=[pltpu.SemaphoreType.DMA((2,))],
        compiler_params=pltpu.CompilerParams(vmem_limit_bytes=1 << 20),
    )(half, full)


def move_rows(packed):
    moved = lax.all_to_all(
        lax.all_to_all(packed, "gy", split_axis=1, concat_axis=1, tiled=True),
        "gx",
        split_axis=0,
        concat_axis=0,
        tiled=True,
    )
    return moved


def move_sums(packed):
    moved = lax.all_to_all(
        lax.all_to_all(packed, "gy", split_axis=1, concat_axis=1, tiled=True),
        "gx",
        split_axis=0,
        concat_axis=0,
        tiled=True,
    )
    return moved


def shards(factor, right_sides, send_rows, neighbour_slot):
    blocks = factor.shape[0]
    width = factor.shape[1]
    far_width = factor.shape[2] - width
    senders = send_rows.shape[1]
    capacity = send_rows.shape[2]
    columns = right_sides.shape[1]
    outer = lax.axis_size("gx")
    inner = lax.axis_size("gy")
    places_all = senders * capacity
    rows_here = blocks * width
    tile = 256
    tiled = capacity % 16 == 0 and (inner * capacity) % 128 == 0
    tiled = tiled and outer > 1 and inner % 2 == 0 and blocks % 2 == 0 and places_all % tile == 0
    if tiled and width % tile == 0 and far_width % 128 == 0 and columns % 128 == 0:
        return fused(factor, right_sides, send_rows, neighbour_slot, tile)
    outgoing = send_rows.reshape(places_all)
    own_factor = factor[:, :, :width]
    far_factor = factor[:, :, width:]
    place_ids = jnp.arange(places_all, dtype=jnp.int32)
    picker = (neighbour_slot[:, :, None] == place_ids[None, None, :]).astype(jnp.bfloat16)
    spread_factor = jnp.einsum(
        "bij,bjs->bis", far_factor, picker, preferred_element_type=jnp.float32
    ).astype(jnp.bfloat16)
    row_ids = jnp.arange(rows_here, dtype=jnp.int32)
    selector = (outgoing[:, None] == row_ids[None, :]).astype(jnp.bfloat16)
    vector = right_sides
    own_rows = vector.reshape(blocks, width, columns)
    packed = jnp.dot(selector, vector, preferred_element_type=jnp.float32).astype(jnp.bfloat16)
    packed = packed.reshape(outer, inner, capacity, columns)
    received = move_rows(packed).reshape(places_all, columns)
    forward = jnp.einsum("bij,bjr->bir", own_factor, own_rows, preferred_element_type=jnp.float32)
    forward = forward + jnp.einsum(
        "bis,sr->bir", spread_factor, received, preferred_element_type=jnp.float32
    )
    weighted = forward.astype(jnp.bfloat16)
    own_back = jnp.einsum("bij,bir->bjr", own_factor, weighted, preferred_element_type=jnp.float32)
    slot_sums = jnp.einsum(
        "bis,bir->sr", spread_factor, weighted, preferred_element_type=jnp.float32
    )
    slot_sums = slot_sums.astype(jnp.bfloat16).reshape(outer, inner, capacity, columns)
    returned = move_sums(slot_sums).reshape(places_all, columns)
    added = jnp.einsum("sk,sr->kr", selector, returned, preferred_element_type=jnp.float32)
    vector = (own_back.reshape(rows_here, columns) + added).astype(jnp.bfloat16)
    return (weighted.reshape(rows_here, columns), vector)


def solution(mesh):
    in_specs = (
        P(("gx", "gy"), None, None),
        P(("gx", "gy"), None),
        P(("gx", "gy"), None, None),
        P(("gx", "gy"), None),
    )
    out_specs = (P(("gx", "gy"), None), P(("gx", "gy"), None))
    return jax.shard_map(shards, mesh=mesh, in_specs=in_specs, out_specs=out_specs, check_vma=False)
```

```python
import functools

import jax
import jax.numpy as jnp
from jax import lax
from jax.experimental import pallas as pl
from jax.experimental.pallas import tpu as pltpu
from jax.sharding import PartitionSpec as P

MESH = pl.DeviceIdType.MESH
NT = (((1,), (1,)), ((), ()))
TN = (((0,), (0,)), ((), ()))


def one_hot(ids, places):
    one, zero = jnp.bfloat16(1), jnp.bfloat16(0)
    return jnp.where(ids == places, one, zero)


def whole(ids):
    return ids.astype(jnp.float32).astype(jnp.bfloat16)


def within(ids, first, size):
    ids = ids - first
    return whole(jnp.where((ids >= 0) & (ids < size), ids, -1))


def count(n, axis):
    shape = (n, 128) if axis == 0 else (16, n)
    return whole(lax.broadcasted_iota(jnp.int32, shape, axis))


def orders(outer):
    split = outer // 2

    def crosses(a, b):
        return (a < split) != (b < split)

    middle, last = (outer - 1) / 2, outer - 1
    rows, sums, waits = [], [], []
    for a in range(outer):
        every = range(outer)
        aside = split <= a < last
        rows.append(
            sorted(
                every,
                key=lambda b: (b == last, aside or abs(b - middle), not crosses(a, b), abs(b - a) if aside else b),
            )
        )
        sums.append(sorted(every, key=lambda b: (b >= split, b if b < split or a in (split - 1, last) else -b)))
        waits.append(sorted((b for b in every if b != a), key=lambda b: (abs(b - a), b)))
    return rows, sums, waits


def kernel(
    outer, inner, tile,
    factor_ref, vector_ref, table_ref, slots_ref, half, full,
    factor, vector, table, slots, spread_t, picker, packed, received, sums, returned,
    id_rows, id_columns, total_t, half_t, wide,
    load_sem, late_sem, go_sem, back_go_sem, come_sem, back_come_sem,
):
    blocks, width, _ = factor.shape
    pairs, _ = vector.shape
    columns = half.shape[1]
    senders, capacity, _ = packed.shape
    places = senders * capacity
    span = inner * capacity
    far_width = slots.shape[1]
    side_blocks = blocks // 2
    gx, gy = lax.axis_index("gx"), lax.axis_index("gy")
    me = gx * inner + gy
    row_order, sum_order, wait_order = orders(outer)

    barrier = pltpu.get_barrier_semaphore()

    def greet(k, carry):
        other = lax.rem(me + k, senders)
        pl.semaphore_signal(
            barrier, inc=1, device_id=(other // inner, lax.rem(other, inner)), device_id_type=MESH
        )
        return carry

    loads = [
        pltpu.make_async_copy(table_ref, table, load_sem.at[0]),
        pltpu.make_async_copy(
            vector_ref.at[pl.ds(0, pairs)], vector.at[:, pl.ds(0, columns)], load_sem.at[1]
        ),
        pltpu.make_async_copy(
            vector_ref.at[pl.ds(pairs, pairs)], vector.at[:, pl.ds(columns, columns)], load_sem.at[2]
        ),
        pltpu.make_async_copy(slots_ref, slots, load_sem.at[3]),
        pltpu.make_async_copy(factor_ref, factor, load_sem.at[4]),
    ]
    for load in loads:
        load.start()
    last = outer - 1
    early = last * inner
    is_last = gx == last
    lax.fori_loop(1, jnp.where(is_last, 1, senders), greet, 0)

    def greet_plane(y, carry):
        pl.semaphore_signal(
            barrier, inc=1, device_id=(gx, lax.rem(gy + y, inner)), device_id_type=MESH
        )
        return carry

    lax.fori_loop(1, jnp.where(is_last, inner, 1), greet_plane, 0)

    def announce(k, carry):
        pl.semaphore_signal(
            late_sem, inc=1, device_id=(k // inner, lax.rem(k, inner)), device_id_type=MESH
        )
        return carry

    def meet():
        @pl.when(is_last)
        def _():
            pl.semaphore_wait(barrier, senders - 1)
            lax.fori_loop(0, early, announce, 0)

        @pl.when(jnp.logical_not(is_last))
        def _():
            pl.semaphore_wait(barrier, early - 1)

    received[me] = jnp.zeros((capacity, columns), jnp.bfloat16)
    returned[me] = jnp.zeros((capacity, columns), jnp.bfloat16)

    def listed(lists, k):
        plane = jnp.int32(lists[outer - 1][k])
        for i in range(outer - 1):
            plane = jnp.where(gx == i, jnp.int32(lists[i][k]), plane)
        return plane

    def group_places(g):
        return pl.ds(pl.multiple_of(g * span, 128), span)

    def group(ref, g):
        return ref[pl.ds(g * inner, inner)].reshape(span, columns)

    def send_group(source, target, send_sem, recv_sem, plane):
        def send(y):
            to_y = lax.rem(gy + inner - y, inner)
            pltpu.make_async_remote_copy(
                src_ref=source.at[plane * inner + to_y],
                dst_ref=target.at[me],
                send_sem=send_sem,
                recv_sem=recv_sem.at[gx],
                device_id=(plane, to_y),
                device_id_type=MESH,
            ).start()

        for y in range(1, inner):
            send(y)

        @pl.when(plane != gx)
        def _():
            send(0)

    def await_bytes(buffer, sem, slabs):
        whole = buffer.at[pl.ds(0, slabs)]
        pltpu.make_async_copy(whole, whole, sem).wait()

    outward = (packed, received, go_sem, come_sem)
    inward = (sums, returned, back_go_sem, back_come_sem)

    loads[0].wait()
    flipped = table[0].T
    for e in range(senders):
        id_columns[pl.ds(e * capacity, capacity), :] = jnp.broadcast_to(
            flipped[:, e : e + 1], (capacity, 128)
        )
    loads[1].wait()
    loads[2].wait()

    def lanes(ids, n):
        return jnp.concatenate([ids] * (n // 128), axis=1)

    def lane_count(n):
        return jnp.concatenate([count(tile, 1)] * (n // 16), axis=0)

    def pack(g):
        part = span // 2
        for r in range(2):
            ids = id_columns[pl.ds(pl.multiple_of(g * span + r * part, 8), part), :]
            upper = ids >= pairs
            ids = jnp.where(upper, ids - pairs, ids)
            rows = jnp.zeros((part, 2 * columns), jnp.float32)
            for c in range(pairs // tile):
                rows = rows + jnp.dot(
                    one_hot(lanes(within(ids, c * tile, tile), tile), lane_count(part)),
                    vector[c * tile : (c + 1) * tile, :],
                    preferred_element_type=jnp.float32,
                )
            upper = lanes(upper.astype(jnp.int32), columns) > 0
            picked = jnp.where(upper, rows[:, columns:], rows[:, :columns])
            packed[pl.ds(g * inner + r * (inner // 2), inner // 2)] = picked.astype(
                jnp.bfloat16
            ).reshape(inner // 2, capacity, columns)

    for k in range(outer):
        plane = listed(row_order, k)
        pack(plane)
        if k == 0:
            meet()

        @pl.when((plane == last) & jnp.logical_not(is_last))
        def _():
            pl.semaphore_wait(late_sem, inner)

        send_group(*outward, plane)

    loads[3].wait()
    loads[4].wait()

    def rows_of(side, b):
        return pl.ds(pl.multiple_of(b * width, width), width), slice(side * columns, (side + 1) * columns)

    def spread_block(side):
        def step(n, carry):
            b = side * side_blocks + n
            here = pl.ds(pl.multiple_of(b * width, width), width)
            far = factor[b, :, width:]
            ids = slots[pl.ds(b, 1), :]
            for c in range(0, places, 1536):
                hot = [
                    one_hot(
                        jnp.broadcast_to(within(ids, d, tile), (tile, far_width)),
                        lanes(count(tile, 0), far_width),
                    )
                    for d in range(c, c + 1536, tile)
                ]
                spread_t[c : c + 1536, here] = lax.dot_general(
                    jnp.concatenate(hot, axis=0), far, NT, preferred_element_type=jnp.float32
                ).astype(jnp.bfloat16)
            total_t[:, here] = lax.dot_general(
                vector[rows_of(side, n)], factor[b, :, :width], (((0,), (1,)), ((), ())),
                preferred_element_type=jnp.float32,
            )
            return carry

        lax.fori_loop(0, side_blocks, step, 0)

    for side in range(2):
        spread_block(side)

    slab = half.shape[0] // 2
    for n in range(outer):
        if n == 0:
            g = gx
            await_bytes(received, come_sem.at[g], inner - 1)
        else:
            g = listed(wait_order, n - 1)
            await_bytes(received, come_sem.at[g], inner)
        rows_t = group(received, g).T
        for h in range(2):
            part = slice(h * slab, (h + 1) * slab)
            value = total_t[:, part] + jnp.dot(
                rows_t, spread_t[group_places(g), part], preferred_element_type=jnp.float32
            )
            if n < outer - 1:
                total_t[:, part] = value
            else:
                half_t[:, part] = value.astype(jnp.bfloat16)

    for k in range(outer):
        g = listed(sum_order, k)
        value = lax.dot_general(
            spread_t[group_places(g), :], half_t[...], NT, preferred_element_type=jnp.float32
        )
        sums[pl.ds(g * inner, inner)] = value.astype(jnp.bfloat16).reshape(inner, capacity, columns)
        send_group(*inward, g)

    def own_block(side):
        def step(n, carry):
            b = side * side_blocks + n
            here = pl.ds(pl.multiple_of(b * width, width), width)
            wide[rows_of(side, n)] = lax.dot_general(
                factor[b, :, :width], half[here, :], TN, preferred_element_type=jnp.float32
            )
            return carry

        lax.fori_loop(0, side_blocks, step, 0)

    half[...] = half_t[...].T
    for side in range(2):
        own_block(side)
    id_rows[...] = jnp.concatenate([table[0, e : e + 1, :] for e in range(senders)], axis=1)
    id_rows[...] = jnp.where(id_rows[...] >= pairs, id_rows[...] - pairs, id_rows[...])

    def pick_rows(n, carry):
        here = pl.ds(pl.multiple_of(n * width, width), width)
        ids = jnp.broadcast_to(within(id_rows[0:1, :], n * width, width), (width, places))
        picker[here, :] = one_hot(ids, lanes(count(width, 0), places))
        return carry

    lax.fori_loop(0, pairs // width, pick_rows, 0)

    await_bytes(packed, go_sem, senders - 1)

    for n in range(outer):
        if n == 0:
            g = gx
            await_bytes(returned, back_come_sem.at[g], inner - 1)
        else:
            g = listed(wait_order, n - 1)
            await_bytes(returned, back_come_sem.at[g], inner)
        rows = group(returned, g)
        upper = lanes(id_columns[pl.ds(pl.multiple_of(g * span, 8), span), :], columns) >= pairs
        none = jnp.zeros_like(rows)
        both = jnp.concatenate([jnp.where(upper, none, rows), jnp.where(upper, rows, none)], axis=1)
        for h in range(2):
            part = pl.ds(h * (pairs // 2), pairs // 2)
            value = wide[part, :] + jnp.dot(
                picker[part, group_places(g)], both, preferred_element_type=jnp.float32
            )
            if n < outer - 1:
                wide[part, :] = value
            else:
                value = value.astype(jnp.bfloat16)
                full[part, :] = value[:, :columns]
                full[pl.ds(pairs + h * (pairs // 2), pairs // 2), :] = value[:, columns:]
    await_bytes(sums, back_go_sem, senders - 1)


def write_out(half_ref, full_ref, half_out, full_out, sems):
    pieces = sems.shape[0] // 2
    size = half_ref.shape[0] // pieces
    copies = [
        pltpu.make_async_copy(
            source.at[pl.ds(n * size, size)], target.at[pl.ds(n * size, size)], sems.at[n + first]
        )
        for source, target, first in ((half_ref, half_out, 0), (full_ref, full_out, pieces))
        for n in range(pieces)
    ]
    for copy in copies:
        copy.start()
    for copy in copies:
        copy.wait()


def fused(factor, right_sides, send_rows, neighbour_slot, tile):
    blocks, width, _ = factor.shape
    rows_here, columns = right_sides.shape
    _, senders, capacity = send_rows.shape
    places = senders * capacity
    outer, inner = lax.axis_size("gx"), lax.axis_size("gy")
    kept = jnp.bfloat16
    out = pltpu.VMEM((rows_here, columns), kept)
    moved = pltpu.VMEM((senders, capacity, columns), kept)
    pairs, far_width = rows_here // 2, neighbour_slot.shape[1]
    flag, flags = pltpu.SemaphoreType.DMA, pltpu.SemaphoreType.DMA((outer,))
    half, full = pl.pallas_call(
        functools.partial(kernel, outer, inner, tile),
        out_shape=(out, out),
        in_specs=[pl.BlockSpec(memory_space=pl.ANY)] * 4,
        out_specs=(pl.BlockSpec(memory_space=pltpu.VMEM),) * 2,
        scratch_shapes=[
            pltpu.VMEM(factor.shape, kept),
            pltpu.VMEM((pairs, 2 * columns), kept),
            pltpu.VMEM(send_rows.shape, jnp.int32),
            pltpu.VMEM(neighbour_slot.shape, jnp.int32),
            pltpu.VMEM((places, rows_here), kept),
            pltpu.VMEM((pairs, places), kept),
            moved, moved, moved, moved,
            pltpu.VMEM((1, places), jnp.int32),
            pltpu.VMEM((places, 128), jnp.int32),
            pltpu.VMEM((columns, rows_here), jnp.float32),
            pltpu.VMEM((columns, rows_here), kept),
            pltpu.VMEM((pairs, 2 * columns), jnp.float32),
            pltpu.SemaphoreType.DMA((5,)),
            pltpu.SemaphoreType.REGULAR,
            flag, flag, flags, flags,
        ],
        compiler_params=pltpu.CompilerParams(collective_id=0, has_side_effects=True),
    )(factor, right_sides, send_rows, neighbour_slot)
    written = jax.ShapeDtypeStruct((rows_here, columns), kept)
    return pl.pallas_call(
        write_out,
        out_shape=(written, written),
        in_specs=[pl.BlockSpec(memory_space=pltpu.VMEM)] * 2,
        out_specs=(pl.BlockSpec(memory_space=pl.ANY),) * 2,
        scratch_shapes=[pltpu.SemaphoreType.DMA((8,))],
        compiler_params=pltpu.CompilerParams(vmem_limit_bytes=1 << 20),
    )(half, full)


def move_rows(packed):
    moved = lax.all_to_all(
        lax.all_to_all(packed, "gy", split_axis=1, concat_axis=1, tiled=True),
        "gx",
        split_axis=0,
        concat_axis=0,
        tiled=True,
    )
    return moved


def move_sums(packed):
    moved = lax.all_to_all(
        lax.all_to_all(packed, "gy", split_axis=1, concat_axis=1, tiled=True),
        "gx",
        split_axis=0,
        concat_axis=0,
        tiled=True,
    )
    return moved


def shards(factor, right_sides, send_rows, neighbour_slot):
    blocks = factor.shape[0]
    width = factor.shape[1]
    far_width = factor.shape[2] - width
    senders = send_rows.shape[1]
    capacity = send_rows.shape[2]
    columns = right_sides.shape[1]
    outer = lax.axis_size("gx")
    inner = lax.axis_size("gy")
    places_all = senders * capacity
    rows_here = blocks * width
    tile = 256
    tiled = capacity % 16 == 0 and (inner * capacity) % 128 == 0
    tiled = tiled and outer > 1 and inner % 2 == 0 and blocks % 2 == 0 and places_all % tile == 0
    if tiled and width % tile == 0 and far_width % 128 == 0 and columns % 128 == 0:
        return fused(factor, right_sides, send_rows, neighbour_slot, tile)
    outgoing = send_rows.reshape(places_all)
    own_factor = factor[:, :, :width]
    far_factor = factor[:, :, width:]
    place_ids = jnp.arange(places_all, dtype=jnp.int32)
    picker = (neighbour_slot[:, :, None] == place_ids[None, None, :]).astype(jnp.bfloat16)
    spread_factor = jnp.einsum(
        "bij,bjs->bis", far_factor, picker, preferred_element_type=jnp.float32
    ).astype(jnp.bfloat16)
    row_ids = jnp.arange(rows_here, dtype=jnp.int32)
    selector = (outgoing[:, None] == row_ids[None, :]).astype(jnp.bfloat16)
    vector = right_sides
    own_rows = vector.reshape(blocks, width, columns)
    packed = jnp.dot(selector, vector, preferred_element_type=jnp.float32).astype(jnp.bfloat16)
    packed = packed.reshape(outer, inner, capacity, columns)
    received = move_rows(packed).reshape(places_all, columns)
    forward = jnp.einsum("bij,bjr->bir", own_factor, own_rows, preferred_element_type=jnp.float32)
    forward = forward + jnp.einsum(
        "bis,sr->bir", spread_factor, received, preferred_element_type=jnp.float32
    )
    weighted = forward.astype(jnp.bfloat16)
    own_back = jnp.einsum("bij,bir->bjr", own_factor, weighted, preferred_element_type=jnp.float32)
    slot_sums = jnp.einsum(
        "bis,bir->sr", spread_factor, weighted, preferred_element_type=jnp.float32
    )
    slot_sums = slot_sums.astype(jnp.bfloat16).reshape(outer, inner, capacity, columns)
    returned = move_sums(slot_sums).reshape(places_all, columns)
    added = jnp.einsum("sk,sr->kr", selector, returned, preferred_element_type=jnp.float32)
    vector = (own_back.reshape(rows_here, columns) + added).astype(jnp.bfloat16)
    return (weighted.reshape(rows_here, columns), vector)


def solution(mesh):
    in_specs = (
        P(("gx", "gy"), None, None),
        P(("gx", "gy"), None),
        P(("gx", "gy"), None, None),
        P(("gx", "gy"), None),
    )
    out_specs = (P(("gx", "gy"), None), P(("gx", "gy"), None))
    return jax.shard_map(shards, mesh=mesh, in_specs=in_specs, out_specs=out_specs, check_vma=False)
```
